256 devices in a mesh: groups: 4 (over x, y), seq: 64 (over z, core).
Axes of the slice: x: 2, y: 2, z: 32, core: 2. Of those that a mesh axis runs over, the one named last changes fastest.
The devices are a block of a 4x8x32 slice.
Arguments:
- img_query: bfloat16 [32, 512, 1536], P('groups', 'seq'), parts along dimension 0, may hold values from -13 to 13
- img_key: bfloat16 [32, 512, 1536], P('groups', 'seq'), parts along dimension 0, may hold values from -5 to 5
- img_value: bfloat16 [32, 512, 1536], P('groups', 'seq'), parts along dimension 0, may hold values from -5 to 5
- txt_key: bfloat16 [32, 256, 1536], P('groups', 'seq'), parts along dimension 0, may hold values from -5 to 5
- txt_value: bfloat16 [32, 256, 1536], P('groups', 'seq'), parts along dimension 0, may hold values from -5 to 5
- txt_len: int32 [32], P('groups'), parts along dimension 0, may hold values from 64 to 256
- slot_of: int32 [32], P('groups'), parts along dimension 0, may hold values from 0 to 7, each once
- step_index: int32 [4], P('groups'), parts along dimension 0, may hold values from 0 to 27
- residual: bfloat16 [32, 512, 1536], P('groups', 'seq'), parts along dimension 0, may hold values from -64 to 64
- modulation: float32 [32, 6, 1536], P('groups'), parts along dimension 0, may hold values from -4 to 4
- out_weight: bfloat16 [1536, 1536], replicated, may hold values from -0.15625 to 0.15625
- out_bias: float32 [1536], replicated, may hold values from -3 to 3
- expand_weight: bfloat16 [3072, 1536], P('seq'), may hold values from -0.15625 to 0.15625
- expand_bias: bfloat16 [3072], P('seq'), may hold values from -3 to 3
- contract_weight: bfloat16 [3072, 1536], P('seq'), may hold values from -0.109375 to 0.109375
- contract_bias: float32 [1536], replicated, may hold values from -3 to 3
- final_weight: bfloat16 [1536, 64], replicated, may hold values from -0.15625 to 0.15625
- final_bias: float32 [64], replicated, may hold values from -3 to 3
- latent: float32 [16, 512, 64], P('groups', 'seq'), parts along dimension 0, may hold values from -6 to 6
Outputs:
- velocity: float32 [16, 512, 64], P('groups', 'seq'), parts along dimension 0
- latent_next: float32 [16, 512, 64], P('groups', 'seq'), parts along dimension 0
The draws below stay inside these ranges and needn't reach their ends.
There are 4 independent parts, one for each index of `groups`. The reference program is written for one: setup_inputs(seed, part) draws one part's arguments, and reference() takes and returns one part's arrays. A program takes and returns all parts, laid end to end along the dimension named above; an argument that names none is the same for every part. Nothing has to cross between parts.
Inputs may be any that keep to these rules, and one draw needn't show every extreme that they name: `slot_of`: each row number appears once.
All inputs are finite; a program needn't handle non-finite values.
Results may differ from the reference program's by a relative error of at most 0.0033.
The reference program's roundings to bfloat16 on the way (of `weights`, `attended`, `ff_in`, `act` and `normed`) count: a program that leaves them out, or rounds other values in their place, can miss the bound.
Values may be sent and summed in bfloat16 or wider, within the bound.
A program may use at most 128 MiB of HBM per device.

```python
import math
import jax
import jax.numpy as jnp
from jax import lax

PROMPTS = 4
BATCH = 8
D = 1536
HEADS = 24
HEAD_DIM = 64
FF = 3072
PATCH = 64
IMG = 512
TXT = 256
NSTEPS = 28


def drawn_pair(key):
    keys_draw = jnp.clip(jax.random.normal(jax.random.fold_in(key, 11), (BATCH, IMG, D), jnp.float32), -4.0, 4.0)
    query_draw = jnp.clip(jax.random.normal(jax.random.fold_in(key, 12), (BATCH, IMG, D), jnp.float32), -4.0, 4.0)
    return (query_draw, keys_draw)


def draw_img_query(key, part):
    return drawn_pair(key)[0].astype(jnp.bfloat16)


def draw_img_key(key, part):
    return drawn_pair(key)[1].astype(jnp.bfloat16)


def draw_residual(key, part):
    drawn = jnp.clip(jax.random.normal(jax.random.fold_in(key, 31), (BATCH, IMG, D), jnp.float32), -6.0, 6.0)
    return drawn.astype(jnp.bfloat16)


def draw_modulation(key, part):
    own = jnp.clip(jax.random.normal(jax.random.fold_in(key, 41), (BATCH, 6, D), jnp.float32), -4.0, 4.0)
    return own


def with_ends(entries, stream_key, smallest, largest):
    dims = entries.shape
    spot = [jax.random.randint(jax.random.fold_in(stream_key, axis), (), 0, dims[axis]) for axis in range(len(dims))]
    entries = entries.at[tuple(spot)].set(smallest)
    longest = dims.index(max(dims))
    spot[longest] = (spot[longest] + 1) % dims[longest]
    return entries.at[tuple(spot)].set(largest)


def shard_levels(key, dims, shards, smallest, top_value):
    factor_of, own = 1.0, jax.random.fold_in(key, 6)
    for dim, blocks in shards:
        steps = jnp.exp(jax.random.uniform(jax.random.fold_in(own, dim), (blocks,), jnp.float32, smallest / len(shards), top_value / len(shards)))
        factor_of = factor_of * jnp.repeat(steps, dims[dim] // blocks).reshape([-1 if axis == dim else 1 for axis in range(len(dims))])
    return factor_of


def scatter_about(rng, extent, deviation, most, pieces=(), held_as=jnp.bfloat16):
    factor_of = shard_levels(rng, extent, pieces, -0.22, 0.18) if pieces else 1.0
    values = jax.random.normal(rng, extent, jnp.float32) * deviation * factor_of
    return jnp.minimum(jnp.maximum(values, -most), most).astype(held_as)


def setup_inputs(seed: int = 0, part: int = 0) -> dict:
    splits = jax.random.split(jax.random.key(seed), 20)
    part_keys = jax.random.split(jax.random.fold_in(splits[19], part), 20)
    img_query = draw_img_query(jax.random.fold_in(jax.random.fold_in(splits[19], part), 71), part)
    img_key = draw_img_key(jax.random.fold_in(jax.random.fold_in(splits[19], part), 71), part)
    img_value = scatter_about(part_keys[2], (BATCH, IMG, D), 1.0, 5.0, ((1, 64),))
    txt_key = scatter_about(part_keys[3], (BATCH, TXT, D), 1.0, 5.0, ((1, 64),))
    txt_value = scatter_about(part_keys[4], (BATCH, TXT, D), 1.0, 5.0, ((1, 64),))
    txt_len = with_ends(jax.random.randint(part_keys[5], (BATCH,), TXT // 4, TXT + 1), jax.random.fold_in(part_keys[5], 1), TXT // 4, TXT).astype(jnp.int32)
    slot_of = jax.random.permutation(part_keys[6], BATCH).astype(jnp.int32)
    step_index = jax.random.randint(part_keys[7], (1,), 0, NSTEPS).astype(jnp.int32)
    residual = draw_residual(jax.random.fold_in(jax.random.fold_in(splits[19], part), 71), part)
    modulation = draw_modulation(jax.random.fold_in(jax.random.fold_in(splits[19], part), 71), part)
    out_weight = scatter_about(splits[10], (D, D), D ** -0.5, 0.15625)
    out_bias = scatter_about(splits[11], (D,), 0.5, 3.0, (), jnp.float32)
    expand_weight = scatter_about(splits[12], (FF, D), D ** -0.5, 0.15625, ((0, 64),))
    expand_bias = scatter_about(splits[13], (FF,), 0.5, 3.0, ((0, 64),))
    contract_weight = scatter_about(splits[14], (FF, D), FF ** -0.5, 0.109375, ((0, 64),))
    contract_bias = scatter_about(splits[15], (D,), 0.5, 3.0, (), jnp.float32)
    final_weight = scatter_about(splits[16], (D, PATCH), D ** -0.5, 0.15625)
    final_bias = scatter_about(splits[17], (PATCH,), 0.5, 3.0, (), jnp.float32)
    latent = scatter_about(part_keys[18], (PROMPTS, IMG, PATCH), 1.0, 6.0, ((1, 64),), jnp.float32)
    return dict(img_query=img_query, img_key=img_key, img_value=img_value, txt_key=txt_key, txt_value=txt_value, txt_len=txt_len, slot_of=slot_of, step_index=step_index, residual=residual, modulation=modulation, out_weight=out_weight, out_bias=out_bias, expand_weight=expand_weight, expand_bias=expand_bias, contract_weight=contract_weight, contract_bias=contract_bias, final_weight=final_weight, final_bias=final_bias, latent=latent)


guidance_scale = 7.0
rescale_mix = 0.7
time_shift = 3.0

def to_items(tensor):
    rows_batch, length, _ = tensor.shape
    return tensor.reshape(rows_batch, length, HEADS, HEAD_DIM).transpose(0, 2, 1, 3).reshape(rows_batch * HEADS, length, HEAD_DIM)

def attend(queries, keys_img, values_img, keys_txt, values_txt, length):
    keys_all = jnp.concatenate([keys_img, keys_txt], axis=0)
    values_all = jnp.concatenate([values_img, values_txt], axis=0)
    scores = jnp.dot(queries, keys_all.T, preferred_element_type=jnp.float32) * (1.0 / math.sqrt(HEAD_DIM))
    column = jnp.arange(keys_all.shape[0], dtype=jnp.int32)
    keep = column < keys_img.shape[0] + length
    scores = jnp.where(keep[None, :], scores, -jnp.inf)
    top_score = lax.optimization_barrier(jnp.max(scores, axis=1, keepdims=True))
    expon = jnp.exp(scores - top_score)
    weights = (expon / lax.optimization_barrier(jnp.sum(expon, axis=1, keepdims=True))).astype(jnp.bfloat16)
    return jnp.dot(weights, values_all, preferred_element_type=jnp.float32).astype(jnp.bfloat16)

def modulate(values, shift, scale):
    centred = values - lax.optimization_barrier(jnp.mean(values, axis=2, keepdims=True))
    variance = lax.optimization_barrier(jnp.mean(centred * centred, axis=2, keepdims=True))
    return (centred * lax.rsqrt(variance + 1e-06) * (1.0 + scale) + shift).astype(jnp.bfloat16)

def sigma_at(time_value):
    return time_shift * time_value / (1.0 + (time_shift - 1.0) * time_value)

def reference(img_query, img_key, img_value, txt_key, txt_value, txt_len, slot_of, step_index, residual, modulation, out_weight, out_bias, expand_weight, expand_bias, contract_weight, contract_bias, final_weight, final_bias, latent):
    rows_batch = img_query.shape[0]
    prompts = rows_batch // 2
    item_len = jnp.repeat(txt_len, HEADS).astype(jnp.int32)
    packed = (to_items(img_query), to_items(img_key), to_items(img_value), to_items(txt_key), to_items(txt_value), item_len)

    def one_item(inputs):
        return attend(*inputs)
    attended = lax.map(one_item, packed)
    attended = attended.reshape(rows_batch, HEADS, IMG, HEAD_DIM).transpose(0, 2, 1, 3).reshape(rows_batch, IMG, D)
    projected = jnp.dot(attended.reshape(rows_batch * IMG, D), out_weight, preferred_element_type=jnp.float32).reshape(rows_batch, IMG, D) + out_bias
    hidden = residual.astype(jnp.float32) + modulation[:, 0:1, :] * projected
    ff_in = modulate(hidden, modulation[:, 1:2, :], modulation[:, 2:3, :])
    pre_act = jnp.dot(ff_in.reshape(rows_batch * IMG, D), expand_weight.T, preferred_element_type=jnp.float32) + expand_bias.astype(jnp.float32)
    act = jax.nn.gelu(pre_act, approximate=True).astype(jnp.bfloat16)
    ff_out = jnp.dot(act, contract_weight, preferred_element_type=jnp.float32).reshape(rows_batch, IMG, D) + contract_bias
    ff_hidden = hidden + modulation[:, 3:4, :] * ff_out
    normed = modulate(ff_hidden, modulation[:, 4:5, :], modulation[:, 5:6, :])
    pred = jnp.dot(normed.reshape(rows_batch * IMG, D), final_weight, preferred_element_type=jnp.float32).reshape(rows_batch, IMG, PATCH) + final_bias
    cond_pred = pred[slot_of[:prompts]]
    uncond_pred = pred[slot_of[prompts:]]
    guided = uncond_pred + guidance_scale * (cond_pred - uncond_pred)
    count = float(IMG * PATCH)
    sum_cond = lax.optimization_barrier(jnp.sum(cond_pred, axis=(1, 2)))
    sq_cond = lax.optimization_barrier(jnp.sum(cond_pred * cond_pred, axis=(1, 2)))
    sum_guided = lax.optimization_barrier(jnp.sum(guided, axis=(1, 2)))
    sq_guided = lax.optimization_barrier(jnp.sum(guided * guided, axis=(1, 2)))
    std_cond = jnp.sqrt((sq_cond - sum_cond * sum_cond / count) / (count - 1.0) + 1e-06)
    std_guided = jnp.sqrt((sq_guided - sum_guided * sum_guided / count) / (count - 1.0) + 1e-06)
    ratio = std_cond / std_guided
    velocity = rescale_mix * ratio[:, None, None] * guided + (1.0 - rescale_mix) * guided
    step_float = step_index[0].astype(jnp.float32)
    delta = sigma_at(1.0 - (step_float + 1.0) / NSTEPS) - sigma_at(1.0 - step_float / NSTEPS)
    latent_next = latent + delta * velocity
    return (velocity, latent_next)
```

```python
import functools
import math

import jax
import jax.numpy as jnp
from jax import lax
from jax.experimental import pallas as pl
from jax.experimental.pallas import tpu as pltpu
from jax.sharding import PartitionSpec as P

HEADS = 24
HEAD_DIM = 64
PATCH = 64
NSTEPS = 28
ITEMS = 3
LANES = 128
MESH = pl.DeviceIdType.MESH

guidance_scale = 7.0
rescale_mix = 0.7
time_shift = 3.0

SENDS_PER_STEP = 63
ATTEND_AT = 12
LAG = 2
CHUNK = 16

f32 = jnp.float32
bf16 = jnp.bfloat16


def sigma_at(time_value):
    return time_shift * time_value / (1.0 + (time_shift - 1.0) * time_value)


def roll(x, shift, axis):
    return pltpu.roll(x, shift, axis)


def modulate(values, shift, scale):
    centred = values - jnp.mean(values, axis=2, keepdims=True)
    variance = jnp.mean(centred * centred, axis=2, keepdims=True)
    return (centred * lax.rsqrt(variance + 1e-06) * (1.0 + scale) + shift)


def kernel(
    sizes,
    txt_len, slot_of, step_index,
    img_query, img_key, img_value, txt_key, txt_value,
    residual, modulation, out_weight, out_bias, expand_weight, expand_bias,
    contract_weight, contract_bias, final_weight, final_bias, latent,
    velocity_out, latent_out,
    wall, ow_v, pack, got, outb, back, attended, bias_all, bias_rows, bias_units, sums_all, hidden, ff_in, acc, pred_v, guided_v,
    in_sem, w_sem, qkv_send, qkv_recv, ret_send, ret_recv, own_recv, x_recv, y_recv, d_recv, sib_recv,
    ring_send, sib_send, x_send, y_send, xr_send, yr_send, bias_send, bias_recv, sums_send, sums_recv,
):
    groups, n, y_size, per_seq = sizes
    chips = n // 2
    half = chips // 2
    g = lax.axis_index("groups")
    me = lax.axis_index("seq")
    core = lax.rem(me, 2)
    sibling = me + 1 - 2 * core
    right = lax.rem(me + 2, n)
    left = lax.rem(me + n - 2, n)
    gy = lax.rem(g, 2)
    gx = lax.rem(g // y_size, 2)
    y_partner = g + 1 - 2 * gy
    x_partner = g + y_size * (1 - 2 * gx)
    q = 2 * gx + gy
    qx = 2 * (1 - gx) + gy
    qy = 2 * gx + 1 - gy
    qd = 3 - q
    width = wall.shape[-1]

    barrier = pltpu.get_barrier_semaphore()

    def greet(j, c):
        pl.semaphore_signal(barrier, inc=1, device_id=(g, lax.rem(me + j, n)), device_id_type=MESH)
        return c

    lax.fori_loop(1, n, greet, 0)
    pl.semaphore_signal(barrier, inc=1, device_id=(x_partner, me), device_id_type=MESH)
    pl.semaphore_signal(barrier, inc=1, device_id=(y_partner, me), device_id_type=MESH)

    own_copies = []
    for part in range(4):
        columns = pl.ds(part * width, width)
        own_copies.append(
            pltpu.make_async_copy(expand_weight.at[:, columns], wall.at[part, 0, me], w_sem.at[part, 0])
        )
        own_copies.append(
            pltpu.make_async_copy(contract_weight.at[:, columns], wall.at[part, 1, me], w_sem.at[part, 1])
        )
    for copy in own_copies:
        copy.start()
    ow_copy = pltpu.make_async_copy(out_weight, ow_v, in_sem.at[0])
    ow_copy.start()

    img_local = img_query.shape[1]
    batch = img_query.shape[0]
    lane = lax.broadcasted_iota(jnp.int32, (batch, 8, LANES), 2)
    sub = lax.broadcasted_iota(jnp.int32, (batch, 8, LANES), 1)
    low = sub < 4
    same = low == (lane < 64)

    def paired(x):
        return jnp.where(same, x, roll(roll(x, 64, 2), 4, 1))

    sub4 = lax.rem(sub, 4)
    for pair in range(HEADS // 2):
        cols = slice(pair * LANES, (pair + 1) * LANES)
        zq = paired(img_query[:, :, cols].astype(f32))
        zk = paired(img_key[:, :, cols].astype(f32))
        zv = paired(img_value[:, :, cols].astype(f32))
        tk = txt_key[:, :, cols].astype(f32)
        tv = txt_value[:, :, cols].astype(f32)
        t = jnp.concatenate([tk, tv], axis=1)
        swapped = roll(t, 64, 2)
        t_same = (sub4 < 2) == (lane < 64)
        zt = jnp.where(t_same, t, jnp.where(sub4 < 2, roll(swapped, 6, 1), roll(swapped, 2, 1)))
        t_even = jnp.where(sub < 6, roll(zt, 4, 1), roll(zt, 2, 1))
        t_odd = jnp.where(sub < 6, roll(zt, 2, 1), zt)
        for odd in range(2):
            head = 2 * pair + odd
            if odd == 0:
                top = jnp.where(low, zq, roll(zk, 4, 1))
                bottom = jnp.where(low, zv, t_even)
            else:
                top = jnp.where(low, roll(zq, 4, 1), zk)
                bottom = jnp.where(low, roll(zv, 4, 1), t_odd)
            block = jnp.concatenate([top, bottom], axis=1).astype(bf16)
            for b in range(batch):
                pack[head % ITEMS, per_seq * b + head // ITEMS] = block[b]

    my_b = me // per_seq
    my_k = lax.rem(me, per_seq)
    bias_all[me] = expand_bias[...]
    for i in range(ITEMS):
        got[i, me] = pack[i, me]

    for copy in own_copies:
        copy.wait()
    pl.semaphore_wait(barrier, n + 1)

    def drain(ref, sem):
        pltpu.make_async_copy(ref, ref, sem).wait()

    def offset(j):
        return jnp.where(lax.rem(j, 2) == 0, n // 2 + j // 2, n // 2 - j // 2)

    def ring(slot, direction, k, to):
        return pltpu.make_async_remote_copy(
            wall.at[q, :, slot], wall.at[q, :, slot], ring_send.at[direction], own_recv.at[direction, k],
            device_id=(g, to), device_id_type=MESH,
        )

    def to_sibling(part, slot):
        return pltpu.make_async_remote_copy(
            wall.at[part, :, slot], wall.at[part, :, slot], sib_send.at[part], sib_recv.at[part],
            device_id=(g, sibling), device_id_type=MESH,
        )

    def across(part, slot, send, recv, partner):
        return pltpu.make_async_remote_copy(
            wall.at[part, :, slot], wall.at[part, :, slot], send, recv,
            device_id=(partner, me), device_id_type=MESH,
        )

    def slot_at(direction, k):
        if direction == 0:
            return lax.rem(me + n - 2 * k, n)
        return lax.rem(me + 2 * k, n)

    ring(me, 0, 1, right).start()
    ring(me, 1, 1, left).start()
    for part in range(4):
        to_sibling(part, me).start()

    def send_bias(j, c):
        peer = lax.rem(me + offset(j), n)
        pltpu.make_async_remote_copy(
            bias_all.at[me], bias_all.at[me], bias_send, bias_recv,
            device_id=(g, peer), device_id_type=MESH,
        ).start()
        return c

    def send_item(index, c):
        i = index // (n - 1)
        peer = lax.rem(me + offset(lax.rem(index, n - 1) + 1), n)
        pltpu.make_async_remote_copy(
            pack.at[i, peer], got.at[i, me], qkv_send.at[i], qkv_recv.at[i],
            device_id=(g, peer), device_id_type=MESH,
        ).start()
        return c

    def attend(i):
        drain(got.at[i, pl.ds(0, n - 1)], qkv_recv.at[i])
        x = got[i].astype(f32)
        top = x[:, 0:8, :].reshape(n // 2, 2, 8, LANES)
        bottom = x[:, 8:16, :].reshape(n // 2, 2, 8, LANES)
        sub_ = lax.broadcasted_iota(jnp.int32, (n // 2, 8, LANES), 1)
        a, b = top[:, 0], top[:, 1]
        c, d = bottom[:, 0], bottom[:, 1]
        qs = jnp.where(sub_ < 4, a, roll(b, 4, 1)).reshape(4 * n, LANES)
        ks = jnp.where(sub_ < 4, roll(a, 4, 1), b).reshape(4 * n, LANES)
        vs = jnp.where(sub_ < 4, c, roll(d, 4, 1)).reshape(4 * n, LANES)
        t = jnp.where(sub_ < 4, roll(c, 4, 1), d).reshape(n // 4, 2, 8, LANES)
        t0, t1 = t[:, 0], t[:, 1]
        sub_t = lax.rem(lax.broadcasted_iota(jnp.int32, (n // 4, 8, LANES), 1), 4)
        tks = jnp.where(sub_t < 2, t0, roll(t1, 2, 1)).reshape(2 * n, LANES)
        tvs = jnp.where(sub_t < 2, roll(t0, 6, 1), t1).reshape(2 * n, LANES)
        kk = jnp.concatenate([ks, tks], axis=0)
        vv = jnp.concatenate([vs, tvs], axis=0)
        keys = jnp.concatenate([kk, roll(kk, 64, 1)], axis=0).astype(bf16)
        vals = jnp.concatenate([vv, roll(vv, 64, 1)], axis=0).astype(bf16)
        rows = 6 * n
        col = lax.broadcasted_iota(jnp.int32, (1, 2 * rows), 1)
        swap = (col >= rows).astype(jnp.int32)
        m = col - swap * rows - 4 * n
        s8 = m % 8
        source = 4 * (m // 8) + 2 * ((s8 % 4) // 2) + s8 // 4
        token = 4 * source + m % 2
        length = txt_len[my_b]
        lane_q = lax.broadcasted_iota(jnp.int32, (4 * n, LANES), 1)
        outs = []
        for side in range(2):
            inside = (lane_q < 64) if side == 0 else (lane_q >= 64)
            qa = jnp.where(inside, qs, 0.0).astype(bf16)
            scores = lax.dot_general(
                qa, keys, (((1,), (1,)), ((), ())), preferred_element_type=f32
            ) * (1.0 / math.sqrt(HEAD_DIM))
            which = swap if side == 0 else 1 - swap
            keep = (m < 0) | (token + 2 * which < length)
            scores = jnp.where(keep, scores, -jnp.inf)
            top_score = jnp.max(scores, axis=1, keepdims=True)
            expon = jnp.exp(scores - top_score)
            weights = (expon / jnp.sum(expon, axis=1, keepdims=True)).astype(bf16)
            outs.append(jnp.dot(weights, vals, preferred_element_type=f32))
        both = jnp.where(lane_q < 64, outs[0], outs[1]).reshape(n // 2, 8, LANES).astype(bf16)
        outb[i] = jnp.stack([both[:, 0:4], both[:, 4:8]], axis=1).reshape(n, 4, LANES)

        def send_back(j, carry):
            peer = lax.rem(me + offset(j), n)
            pltpu.make_async_remote_copy(
                outb.at[i, peer], back.at[i, me], ret_send.at[i], ret_recv.at[i],
                device_id=(g, peer), device_id_type=MESH,
            ).start()
            return carry

        lax.fori_loop(1, n, send_back, 0)
        back[i, me] = outb[i, me]

    def step(k, carry):
        total = ITEMS * (n - 1)
        first = (k - 1) * SENDS_PER_STEP

        @pl.when(first < total)
        def _():
            lax.fori_loop(0, SENDS_PER_STEP, lambda s, c: send_item(first + s, c), 0)

        @pl.when(k == 4)
        def _():
            lax.fori_loop(1, n, send_bias, 0)

        for direction, last, onward in ((0, half, right), (1, half - 1, left)):

            @pl.when(k <= last)
            def _():
                slot = slot_at(direction, k)
                ring(slot, direction, k, onward).wait_recv()

                @pl.when(k < last)
                def _():
                    ring(slot, direction, k + 1, onward).start()

                across(q, slot, x_send, x_recv.at[direction, k], x_partner).start()
                across(q, slot, y_send, y_recv.at[direction, k], y_partner).start()
                to_sibling(q, slot).start()

        for direction, last in ((0, half), (1, half - 1)):
            late = k - LAG

            @pl.when((late >= 1) & (late <= last))
            def _():
                slot = slot_at(direction, late)
                across(qx, slot, x_send, x_recv.at[direction, late], x_partner).wait_recv()
                if direction == 0:
                    across(qx, slot, yr_send, d_recv.at[direction, late], y_partner).start()
                to_sibling(qx, slot).start()
                across(qy, slot, y_send, y_recv.at[direction, late], y_partner).wait_recv()
                if direction == 1:
                    across(qy, slot, xr_send, d_recv.at[direction, late], x_partner).start()
                to_sibling(qy, slot).start()

            later = k - 2 * LAG

            @pl.when((later >= 1) & (later <= last))
            def _():
                slot = slot_at(direction, later)
                across(qd, slot, xr_send, d_recv.at[direction, later], x_partner).wait_recv()
                to_sibling(qd, slot).start()

        at = k - ATTEND_AT

        @pl.when((at >= 0) & (lax.rem(at, 2) == 0) & (at // 2 < ITEMS))
        def _():
            attend(at // 2)

        return carry

    lax.fori_loop(1, half + 2 * LAG + 1, step, 0)

    chunks = len(range(0, n, CHUNK))
    hidden_own = wall.shape[3]
    chunk_units = CHUNK * hidden_own
    drain(bias_all.at[pl.ds(0, n - 1)], bias_recv)
    for r in range(n):
        bias_rows[r : r + 1, :] = bias_all[r]
    unit = lax.broadcasted_iota(jnp.int32, (LANES, chunk_units), 1)
    block_of = ((unit.astype(f32) + 0.5) * (1.0 / hidden_own)).astype(jnp.int32)
    pick = jnp.where(
        unit - block_of * hidden_own == lax.broadcasted_iota(jnp.int32, (LANES, chunk_units), 0), 1.0, 0.0
    ).astype(bf16)
    mine = block_of[:CHUNK] == lax.broadcasted_iota(jnp.int32, (CHUNK, chunk_units), 0)
    for c in range(chunks):
        spread = jnp.dot(
            bias_rows[c * CHUNK : (c + 1) * CHUNK, :].astype(bf16), pick, preferred_element_type=f32
        )
        bias_units[c] = jnp.sum(jnp.where(mine, spread, 0.0), axis=0, keepdims=True)

    for i in range(ITEMS):
        drain(back.at[i, pl.ds(0, n - 1)], ret_recv.at[i])
    for pair in range(HEADS // 2):
        cols = slice(pair * LANES, (pair + 1) * LANES)
        halves = []
        for head in (2 * pair, 2 * pair + 1):
            i, k = head % ITEMS, head // ITEMS
            halves.append(jnp.stack([back[i, per_seq * b + k].astype(f32) for b in range(batch)], axis=0))
        z = jnp.concatenate(halves, axis=1)
        attended[:, cols] = paired(z).reshape(batch * img_local, LANES).astype(bf16)

    ow_copy.wait()
    d_model = attended.shape[-1]
    shape3 = (batch, img_local, d_model)
    projected = jnp.dot(attended[...], ow_v[...], preferred_element_type=f32).reshape(shape3) + out_bias[...]
    hidden[...] = residual[...].astype(f32) + modulation[:, 0:1, :] * projected
    ff_in[...] = (
        modulate(hidden[...], modulation[:, 1:2, :], modulation[:, 2:3, :])
        .reshape(batch * img_local, d_model)
        .astype(bf16)
    )
    acc[...] = jnp.zeros_like(acc)

    for part in range(4):
        drain(wall.at[part, :, pl.ds(0, chips)], sib_recv.at[part])

    def feed(c, carry):
        blocks = pl.ds(c * CHUNK, CHUNK)
        pre = bias_units[c]
        for part in range(4):
            w = wall[part, 0, blocks].reshape(chunk_units, width)
            pre = pre + lax.dot_general(
                ff_in[:, part * width : (part + 1) * width], w,
                (((1,), (1,)), ((), ())), preferred_element_type=f32,
            )
        act = (0.5 * pre * (1.0 + jnp.tanh(math.sqrt(2.0 / math.pi) * (pre + 0.044715 * pre * pre * pre)))).astype(bf16)
        for part in range(4):
            w = wall[part, 1, blocks].reshape(chunk_units, width)
            acc[:, part * width : (part + 1) * width] += jnp.dot(act, w, preferred_element_type=f32)
        return carry

    lax.fori_loop(0, chunks, feed, 0)

    ff_hidden = hidden[...] + modulation[:, 3:4, :] * (acc[...].reshape(shape3) + contract_bias[...])
    normed = (
        modulate(ff_hidden, modulation[:, 4:5, :], modulation[:, 5:6, :])
        .reshape(batch * img_local, d_model)
        .astype(bf16)
    )
    pred = jnp.dot(normed, final_weight[...], preferred_element_type=f32) + final_bias[...]
    pred_v[...] = pred.reshape(batch, img_local, PATCH)
    prompts = batch // 2
    lane_row = lax.broadcasted_iota(jnp.int32, (1, LANES), 1)
    row = jnp.zeros((1, LANES), f32)

    def full_sum(x):
        return jnp.sum(jnp.sum(x, axis=1, keepdims=True), axis=0, keepdims=True)

    for p in range(prompts):
        cond = pred_v[slot_of[p]]
        uncond = pred_v[slot_of[prompts + p]]
        guided = uncond + guidance_scale * (cond - uncond)
        guided_v[p] = guided
        for s, value in enumerate((cond, cond * cond, guided, guided * guided)):
            row = jnp.where(lane_row == s * prompts + p, full_sum(value), row)
    sums_all[me] = row

    def send_sums(j, c):
        peer = lax.rem(me + offset(j), n)
        pltpu.make_async_remote_copy(
            sums_all.at[me], sums_all.at[me], sums_send, sums_recv,
            device_id=(g, peer), device_id_type=MESH,
        ).start()
        return c

    lax.fori_loop(1, n, send_sums, 0)

    for direction, count in ((0, half), (1, half - 1)):
        drain(wall.at[0, :, pl.ds(0, count)], ring_send.at[direction])
    for part in range(4):
        drain(wall.at[part, :, pl.ds(0, chips)], sib_send.at[part])
    drain(wall.at[0, :, pl.ds(0, chips - 1)], x_send)
    drain(wall.at[0, :, pl.ds(0, chips - 1)], y_send)
    drain(wall.at[0, :, pl.ds(0, half - 1)], xr_send)
    drain(wall.at[0, :, pl.ds(0, half)], yr_send)
    drain(bias_all.at[pl.ds(0, n - 1)], bias_send)
    for i in range(ITEMS):
        drain(pack.at[i, pl.ds(0, n - 1)], qkv_send.at[i])
        drain(outb.at[i, pl.ds(0, n - 1)], ret_send.at[i])
    drain(sums_all.at[pl.ds(0, n - 1)], sums_recv)
    drain(sums_all.at[pl.ds(0, n - 1)], sums_send)

    totals = jnp.sum(sums_all[...], axis=0)
    count = float(img_local * n * PATCH)
    step_float = jnp.full((img_local, PATCH), step_index[0], jnp.int32).astype(f32)
    delta = sigma_at(1.0 - (step_float + 1.0) / NSTEPS) - sigma_at(1.0 - step_float / NSTEPS)
    for p in range(prompts):
        t = [totals[:, s * prompts + p : s * prompts + p + 1] for s in range(4)]
        std_cond = jnp.sqrt((t[1] - t[0] * t[0] / count) / (count - 1.0) + 1e-06)
        std_guided = jnp.sqrt((t[3] - t[2] * t[2] / count) / (count - 1.0) + 1e-06)
        ratio = std_cond / std_guided
        guided = guided_v[p]
        velocity = rescale_mix * ratio * guided + (1.0 - rescale_mix) * guided
        velocity_out[p] = velocity
        latent_out[p] = latent[p] + delta * velocity


def body(
    y_size,
    groups,
    n,
    img_query,
    img_key,
    img_value,
    txt_key,
    txt_value,
    txt_len,
    slot_of,
    step_index,
    residual,
    modulation,
    out_weight,
    out_bias,
    expand_weight,
    expand_bias,
    contract_weight,
    contract_bias,
    final_weight,
    final_bias,
    latent,
):
    batch, img_local, d_model = img_query.shape
    prompts = batch // 2
    hidden_own = expand_weight.shape[0]
    per_seq = n // batch
    rows = batch * img_local
    bias_row = jnp.pad(expand_bias.astype(f32), (0, LANES - hidden_own)).reshape(1, LANES)
    vmem = pl.BlockSpec(memory_space=pltpu.VMEM)
    smem = pl.BlockSpec(memory_space=pltpu.SMEM)
    hbm = pl.BlockSpec(memory_space=pl.ANY)
    dma = pltpu.SemaphoreType.DMA
    half = n // 4
    return pl.pallas_call(
        functools.partial(kernel, (groups, n, y_size, per_seq)),
        out_shape=(jax.ShapeDtypeStruct(latent.shape, f32), jax.ShapeDtypeStruct(latent.shape, f32)),
        in_specs=[smem] * 3 + [vmem] * 7 + [hbm, vmem, hbm, vmem, hbm] + [vmem] * 4,
        out_specs=(vmem, vmem),
        scratch_shapes=[
            pltpu.VMEM((4, 2, n, hidden_own, d_model // 4), bf16),
            pltpu.VMEM((d_model, d_model), bf16),
            pltpu.VMEM((ITEMS, n, 16, LANES), bf16),
            pltpu.VMEM((ITEMS, n, 16, LANES), bf16),
            pltpu.VMEM((ITEMS, n, 4, LANES), bf16),
            pltpu.VMEM((ITEMS, n, 4, LANES), bf16),
            pltpu.VMEM((rows, d_model), bf16),
            pltpu.VMEM((n, 1, LANES), f32),
            pltpu.VMEM((n, LANES), f32),
            pltpu.VMEM((n // CHUNK, 1, CHUNK * hidden_own), f32),
            pltpu.VMEM((n, 1, LANES), f32),
            pltpu.VMEM((batch, img_local, d_model), f32),
            pltpu.VMEM((rows, d_model), bf16),
            pltpu.VMEM((rows, d_model), f32),
            pltpu.VMEM((batch, img_local, PATCH), f32),
            pltpu.VMEM((prompts, img_local, PATCH), f32),
            dma((1,)),
            dma((4, 2)),
            dma((ITEMS,)),
            dma((ITEMS,)),
            dma((ITEMS,)),
            dma((ITEMS,)),
            dma((2, half + 1)),
            dma((2, half + 1)),
            dma((2, half + 1)),
            dma((2, half + 1)),
            dma((4,)),
            dma((2,)),
            dma((4,)),
            dma,
            dma,
            dma,
            dma,
            dma,
            dma,
            dma,
            dma,
        ],
        compiler_params=pltpu.CompilerParams(
            collective_id=0, has_side_effects=True, vmem_limit_bytes=60 * 1024 * 1024
        ),
    )(
        txt_len, slot_of, step_index,
        img_query, img_key, img_value, txt_key, txt_value,
        residual, modulation, out_weight, out_bias.reshape(1, -1), expand_weight, bias_row,
        contract_weight, contract_bias.reshape(1, -1), final_weight, final_bias.reshape(1, -1), latent,
    )


def solution(mesh):
    in_specs = (
        P("groups", "seq", None),
        P("groups", "seq", None),
        P("groups", "seq", None),
        P("groups", "seq", None),
        P("groups", "seq", None),
        P("groups"),
        P("groups"),
        P("groups"),
        P("groups", "seq", None),
        P("groups", None, None),
        P(),
        P(),
        P("seq", None),
        P("seq"),
        P("seq", None),
        P(),
        P(),
        P(),
        P("groups", "seq", None),
    )
    out_specs = (P("groups", "seq", None), P("groups", "seq", None))
    groups, n = mesh.shape["groups"], mesh.shape["seq"]
    bits = groups.bit_length() - 1
    y_size = 1 << (bits - bits // 2)
    return jax.shard_map(
        functools.partial(body, y_size, groups, n),
        mesh=mesh, in_specs=in_specs, out_specs=out_specs, check_vma=False,
    )
```

```python
import functools
import math

import jax
import jax.numpy as jnp
from jax import lax
from jax.experimental import pallas as pl
from jax.experimental.pallas import tpu as pltpu
from jax.sharding import PartitionSpec as P

HEADS = 24
HEAD_DIM = 64
PATCH = 64
NSTEPS = 28
ITEMS = 3
LANES = 128
MESH = pl.DeviceIdType.MESH

guidance_scale = 7.0
rescale_mix = 0.7
time_shift = 3.0

SENDS_PER_STEP = 13
ATTEND_AT = (7, 12, 17)
LAG = 3
CHUNK = 16

f32 = jnp.float32
bf16 = jnp.bfloat16


def sigma_at(time_value):
    return time_shift * time_value / (1.0 + (time_shift - 1.0) * time_value)


def roll(x, shift, axis):
    return pltpu.roll(x, shift, axis)


def modulate(values, shift, scale):
    centred = values - jnp.mean(values, axis=2, keepdims=True)
    variance = jnp.mean(centred * centred, axis=2, keepdims=True)
    return (centred * lax.rsqrt(variance + 1e-06) * (1.0 + scale) + shift)


def kernel(
    sizes,
    expand_weight, contract_weight, arrays, results, held,
    wall, pack, got, outb, back, attended, bias_all, bias_rows, bias_units, sums_all, hidden, ff_in, acc, pred_v, guided_v,
    in_sem, w_sem, qkv_send, qkv_recv, ret_send, ret_recv, own_recv, x_recv, y_recv, d_recv, sib_recv,
    ring_send, sib_send, x_send, y_send, xr_send, yr_send, bias_send, bias_recv, sums_send, sums_recv,
):
    groups, n, y_size, per_seq = sizes
    (
        img_query, img_key, img_value, txt_key, txt_value, expand_bias, txt_len,
        slot_of, step_index, residual, modulation, ow_v, out_bias, contract_bias, final_weight, final_bias, latent,
    ) = held
    early = 7
    chips = n // 2
    half = chips // 2
    g = lax.axis_index("groups")
    me = lax.axis_index("seq")
    core = lax.rem(me, 2)
    sibling = me + 1 - 2 * core
    right = lax.rem(me + 2, n)
    left = lax.rem(me + n - 2, n)
    gy = lax.rem(g, 2)
    gx = lax.rem(g // y_size, 2)
    y_partner = g + 1 - 2 * gy
    x_partner = g + y_size * (1 - 2 * gx)
    q = 2 * gx + gy
    qx = 2 * (1 - gx) + gy
    qy = 2 * gx + 1 - gy
    qd = 3 - q
    width = wall.shape[-1]

    barrier = pltpu.get_barrier_semaphore()

    def greet(j, c):
        pl.semaphore_signal(barrier, inc=1, device_id=(g, lax.rem(me + j, n)), device_id_type=MESH)
        return c

    lax.fori_loop(1, n, greet, 0)
    pl.semaphore_signal(barrier, inc=1, device_id=(x_partner, me), device_id_type=MESH)
    pl.semaphore_signal(barrier, inc=1, device_id=(y_partner, me), device_id_type=MESH)

    in_copies = [pltpu.make_async_copy(a, h, in_sem.at[i]) for i, (a, h) in enumerate(zip(arrays, held))]
    for copy in in_copies:
        copy.start()
    own_copies = []
    for part in range(4):
        columns = pl.ds(part * width, width)
        own_copies.append(
            pltpu.make_async_copy(expand_weight.at[:, columns], wall.at[part, 0, me], w_sem.at[part, 0])
        )
        own_copies.append(
            pltpu.make_async_copy(contract_weight.at[:, columns], wall.at[part, 1, me], w_sem.at[part, 1])
        )
    for copy in own_copies:
        copy.start()
    for copy in in_copies[:early]:
        copy.wait()

    img_local = img_query.shape[1]
    batch = img_query.shape[0]
    lane = lax.broadcasted_iota(jnp.int32, (batch, 8, LANES), 2)
    sub = lax.broadcasted_iota(jnp.int32, (batch, 8, LANES), 1)
    low = sub < 4
    same = low == (lane < 64)

    def paired(x):
        return jnp.where(same, x, roll(roll(x, 64, 2), 4, 1))

    sub4 = lax.rem(sub, 4)
    for pair in range(HEADS // 2):
        cols = slice(pair * LANES, (pair + 1) * LANES)
        zq = paired(img_query[:, :, cols].astype(f32))
        zk = paired(img_key[:, :, cols].astype(f32))
        zv = paired(img_value[:, :, cols].astype(f32))
        tk = txt_key[:, :, cols].astype(f32)
        tv = txt_value[:, :, cols].astype(f32)
        t = jnp.concatenate([tk, tv], axis=1)
        swapped = roll(t, 64, 2)
        t_same = (sub4 < 2) == (lane < 64)
        zt = jnp.where(t_same, t, jnp.where(sub4 < 2, roll(swapped, 6, 1), roll(swapped, 2, 1)))
        t_even = jnp.where(sub < 6, roll(zt, 4, 1), roll(zt, 2, 1))
        t_odd = jnp.where(sub < 6, roll(zt, 2, 1), zt)
        for odd in range(2):
            head = 2 * pair + odd
            if odd == 0:
                top = jnp.where(low, zq, roll(zk, 4, 1))
                bottom = jnp.where(low, zv, t_even)
            else:
                top = jnp.where(low, roll(zq, 4, 1), zk)
                bottom = jnp.where(low, roll(zv, 4, 1), t_odd)
            block = jnp.concatenate([top, bottom], axis=1).astype(bf16)
            for b in range(batch):
                pack[head % ITEMS, per_seq * b + head // ITEMS] = block[b]

    my_b = me // per_seq
    my_k = lax.rem(me, per_seq)
    bias_all[me] = jnp.zeros((1, LANES), f32)
    bias_all[me, 0:1, 0 : expand_bias.shape[0]] = expand_bias[...].astype(f32).reshape(1, -1)
    for i in range(ITEMS):
        got[i, me] = pack[i, me]

    for copy in own_copies:
        copy.wait()
    with jax.named_scope("barrier"):
        pl.semaphore_wait(barrier, n + 1)

    def drain(ref, sem):
        pltpu.make_async_copy(ref, ref, sem).wait()

    scope = jax.named_scope

    def offset(j):
        return jnp.where(lax.rem(j, 2) == 0, n // 2 + j // 2, n // 2 - j // 2)

    def ring(slot, direction, k, to):
        return pltpu.make_async_remote_copy(
            wall.at[q, :, slot], wall.at[q, :, slot], ring_send.at[direction], own_recv.at[direction, k],
            device_id=(g, to), device_id_type=MESH,
        )

    def to_sibling(part, slot):
        return pltpu.make_async_remote_copy(
            wall.at[part, :, slot], wall.at[part, :, slot], sib_send.at[part], sib_recv.at[part],
            device_id=(g, sibling), device_id_type=MESH,
        )

    def across(part, slot, send, recv, partner):
        return pltpu.make_async_remote_copy(
            wall.at[part, :, slot], wall.at[part, :, slot], send, recv,
            device_id=(partner, me), device_id_type=MESH,
        )

    def slot_at(direction, k):
        if direction == 0:
            return lax.rem(me + n - 2 * k, n)
        return lax.rem(me + 2 * k, n)

    ring(me, 0, 1, right).start()
    ring(me, 1, 1, left).start()
    for part in range(4):
        to_sibling(part, me).start()

    def send_bias(j, c):
        peer = lax.rem(me + offset(j), n)
        pltpu.make_async_remote_copy(
            bias_all.at[me], bias_all.at[me], bias_send, bias_recv,
            device_id=(g, peer), device_id_type=MESH,
        ).start()
        return c

    def send_item(index, c):
        i = index // (n - 1)
        peer = lax.rem(me + offset(lax.rem(index, n - 1) + 1), n)
        pltpu.make_async_remote_copy(
            pack.at[i, peer], got.at[i, me], qkv_send.at[i], qkv_recv.at[i],
            device_id=(g, peer), device_id_type=MESH,
        ).start()
        return c

    def attend(i):
        with scope("items"):
            drain(got.at[i, pl.ds(0, n - 1)], qkv_recv.at[i])
        x = got[i].astype(f32)
        top = x[:, 0:8, :].reshape(n // 2, 2, 8, LANES)
        bottom = x[:, 8:16, :].reshape(n // 2, 2, 8, LANES)
        sub_ = lax.broadcasted_iota(jnp.int32, (n // 2, 8, LANES), 1)
        a, b = top[:, 0], top[:, 1]
        c, d = bottom[:, 0], bottom[:, 1]
        qs = jnp.where(sub_ < 4, a, roll(b, 4, 1)).reshape(4 * n, LANES)
        ks = jnp.where(sub_ < 4, roll(a, 4, 1), b).reshape(4 * n, LANES)
        vs = jnp.where(sub_ < 4, c, roll(d, 4, 1)).reshape(4 * n, LANES)
        t = jnp.where(sub_ < 4, roll(c, 4, 1), d).reshape(n // 4, 2, 8, LANES)
        t0, t1 = t[:, 0], t[:, 1]
        sub_t = lax.rem(lax.broadcasted_iota(jnp.int32, (n // 4, 8, LANES), 1), 4)
        tks = jnp.where(sub_t < 2, t0, roll(t1, 2, 1)).reshape(2 * n, LANES)
        tvs = jnp.where(sub_t < 2, roll(t0, 6, 1), t1).reshape(2 * n, LANES)
        kk = jnp.concatenate([ks, tks], axis=0)
        vv = jnp.concatenate([vs, tvs], axis=0)
        keys = jnp.concatenate([kk, roll(kk, 64, 1)], axis=0).astype(bf16)
        vals = jnp.concatenate([vv, roll(vv, 64, 1)], axis=0).astype(bf16)
        img, rows = 4 * n, 6 * n
        m = lax.broadcasted_iota(jnp.int32, (1, 2 * n), 1)
        s8 = m % 8
        token = 4 * (4 * (m // 8) + 2 * ((s8 % 4) // 2) + s8 // 4) + m % 2
        length = txt_len[my_b]
        lane_q = lax.broadcasted_iota(jnp.int32, (4 * n, LANES), 1)
        scale = 1.0 / math.sqrt(HEAD_DIM)
        outs = []
        for side in range(2):
            inside = (lane_q < 64) if side == 0 else (lane_q >= 64)
            qa = jnp.where(inside, qs * scale, 0.0).astype(bf16)
            scores = lax.dot_general(qa, keys, (((1,), (1,)), ((), ())), preferred_element_type=f32)
            pieces = []
            for swap in range(2):
                which = swap if side == 0 else 1 - swap
                pieces.append(scores[:, swap * rows : swap * rows + img])
                text = scores[:, swap * rows + img : (swap + 1) * rows]
                pieces.append(jnp.where(token + 2 * which < length, text, -jnp.inf))
            scores = jnp.concatenate(pieces, axis=1)
            top_score = jnp.max(scores, axis=1, keepdims=True)
            expon = jnp.exp(scores - top_score)
            weights = (expon * (1.0 / jnp.sum(expon, axis=1, keepdims=True))).astype(bf16)
            outs.append(jnp.dot(weights, vals, preferred_element_type=f32))
        both = jnp.where(lane_q < 64, outs[0], outs[1]).reshape(n // 2, 8, LANES).astype(bf16)
        outb[i] = jnp.stack([both[:, 0:4], both[:, 4:8]], axis=1).reshape(n, 4, LANES)

        def send_back(j, carry):
            peer = lax.rem(me + offset(j), n)
            pltpu.make_async_remote_copy(
                outb.at[i, peer], back.at[i, me], ret_send.at[i], ret_recv.at[i],
                device_id=(g, peer), device_id_type=MESH,
            ).start()
            return carry

        lax.fori_loop(1, n, send_back, 0)
        back[i, me] = outb[i, me]

    def step(k, carry):
        total = ITEMS * (n - 1)
        first = (k - 1) * SENDS_PER_STEP

        @pl.when(first < total)
        def _():
            with scope("send"):
                lax.fori_loop(first, jnp.minimum(first + SENDS_PER_STEP, total), send_item, 0)

        @pl.when(k == 4)
        def _():
            lax.fori_loop(1, n, send_bias, 0)

        for direction, last, onward in ((0, half, right), (1, half - 1, left)):

            @pl.when(k <= last)
            def _():
                slot = slot_at(direction, k)
                with scope("own"):
                    ring(slot, direction, k, onward).wait_recv()

                @pl.when(k < last)
                def _():
                    ring(slot, direction, k + 1, onward).start()

                across(q, slot, x_send, x_recv.at[direction, k], x_partner).start()
                across(q, slot, y_send, y_recv.at[direction, k], y_partner).start()
                to_sibling(q, slot).start()

        for direction, last in ((0, half), (1, half - 1)):
            late = k - LAG

            @pl.when((late >= 1) & (late <= last))
            def _():
                slot = slot_at(direction, late)
                with scope("x"):
                    across(qx, slot, x_send, x_recv.at[direction, late], x_partner).wait_recv()
                if direction == 0:
                    across(qx, slot, yr_send, d_recv.at[direction, late], y_partner).start()
                to_sibling(qx, slot).start()
                with scope("y"):
                    across(qy, slot, y_send, y_recv.at[direction, late], y_partner).wait_recv()
                if direction == 1:
                    across(qy, slot, xr_send, d_recv.at[direction, late], x_partner).start()
                to_sibling(qy, slot).start()

            later = k - 2 * LAG

            @pl.when((later >= 1) & (later <= last))
            def _():
                slot = slot_at(direction, later)
                with scope("d"):
                    across(qd, slot, xr_send, d_recv.at[direction, later], x_partner).wait_recv()
                to_sibling(qd, slot).start()

        first_at, second_at, third_at = ATTEND_AT

        @pl.when((k == first_at) | (k == second_at) | (k == third_at))
        def _():
            with scope("attend"):
                attend((k >= second_at).astype(jnp.int32) + (k >= third_at).astype(jnp.int32))

        return carry

    lax.fori_loop(1, half + 2 * LAG + 1, step, 0)

    chunks = len(range(0, n, CHUNK))
    hidden_own = wall.shape[3]
    chunk_units = CHUNK * hidden_own
    drain(bias_all.at[pl.ds(0, n - 1)], bias_recv)
    for r in range(n):
        bias_rows[r : r + 1, :] = bias_all[r]
    unit = lax.broadcasted_iota(jnp.int32, (LANES, chunk_units), 1)
    block_of = ((unit.astype(f32) + 0.5) * (1.0 / hidden_own)).astype(jnp.int32)
    pick = jnp.where(
        unit - block_of * hidden_own == lax.broadcasted_iota(jnp.int32, (LANES, chunk_units), 0), 1.0, 0.0
    ).astype(bf16)
    mine = block_of[:CHUNK] == lax.broadcasted_iota(jnp.int32, (CHUNK, chunk_units), 0)
    for c in range(chunks):
        spread = jnp.dot(
            bias_rows[c * CHUNK : (c + 1) * CHUNK, :].astype(bf16), pick, preferred_element_type=f32
        )
        bias_units[c] = jnp.sum(jnp.where(mine, spread, 0.0), axis=0, keepdims=True)

    for i in range(ITEMS):
        with scope("ret"):
            drain(back.at[i, pl.ds(0, n - 1)], ret_recv.at[i])
    for pair in range(HEADS // 2):
        cols = slice(pair * LANES, (pair + 1) * LANES)
        halves = []
        for head in (2 * pair, 2 * pair + 1):
            i, k = head % ITEMS, head // ITEMS
            halves.append(jnp.stack([back[i, per_seq * b + k].astype(f32) for b in range(batch)], axis=0))
        z = jnp.concatenate(halves, axis=1)
        attended[:, cols] = paired(z).reshape(batch * img_local, LANES).astype(bf16)

    for copy in in_copies[early:]:
        copy.wait()
    d_model = attended.shape[-1]
    shape3 = (batch, img_local, d_model)
    projected = jnp.dot(attended[...], ow_v[...], preferred_element_type=f32).reshape(shape3) + out_bias[...].reshape(1, 1, -1)
    hidden[...] = residual[...].astype(f32) + modulation[0][:, None, :] * projected
    ff_in[...] = (
        modulate(hidden[...], modulation[1][:, None, :], modulation[2][:, None, :])
        .reshape(batch * img_local, d_model)
        .astype(bf16)
    )
    acc[...] = jnp.zeros_like(acc)

    for part in range(4):
        with scope("sib"):
            drain(wall.at[part, :, pl.ds(0, chips)], sib_recv.at[part])

    def feed(c, carry):
        blocks = pl.ds(c * CHUNK, CHUNK)
        pre = bias_units[c]
        for part in range(4):
            w = wall[part, 0, blocks].reshape(chunk_units, width)
            pre = pre + lax.dot_general(
                ff_in[:, part * width : (part + 1) * width], w,
                (((1,), (1,)), ((), ())), preferred_element_type=f32,
            )
        act = (0.5 * pre * (1.0 + jnp.tanh(math.sqrt(2.0 / math.pi) * (pre + 0.044715 * pre * pre * pre)))).astype(bf16)
        for part in range(4):
            w = wall[part, 1, blocks].reshape(chunk_units, width)
            acc[:, part * width : (part + 1) * width] += jnp.dot(act, w, preferred_element_type=f32)
        return carry

    with scope("ffn"):
        lax.fori_loop(0, chunks, feed, 0)

    ff_hidden = hidden[...] + modulation[3][:, None, :] * (acc[...].reshape(shape3) + contract_bias[...].reshape(1, 1, -1))
    normed = (
        modulate(ff_hidden, modulation[4][:, None, :], modulation[5][:, None, :])
        .reshape(batch * img_local, d_model)
        .astype(bf16)
    )
    pred = lax.dot_general(
        normed, final_weight[...], (((1,), (1,)), ((), ())), preferred_element_type=f32
    ) + final_bias[...].reshape(1, -1)
    pred_v[...] = pred.reshape(batch, img_local, PATCH)
    prompts = batch // 2
    lane_row = lax.broadcasted_iota(jnp.int32, (1, LANES), 1)
    row = jnp.zeros((1, LANES), f32)

    def full_sum(x):
        return jnp.sum(jnp.sum(x, axis=1, keepdims=True), axis=0, keepdims=True)

    for p in range(prompts):
        cond = pred_v[slot_of[p]]
        uncond = pred_v[slot_of[prompts + p]]
        guided = uncond + guidance_scale * (cond - uncond)
        guided_v[p] = guided
        for s, value in enumerate((cond, cond * cond, guided, guided * guided)):
            row = jnp.where(lane_row == s * prompts + p, full_sum(value), row)
    sums_all[me] = row

    def send_sums(j, c):
        peer = lax.rem(me + offset(j), n)
        pltpu.make_async_remote_copy(
            sums_all.at[me], sums_all.at[me], sums_send, sums_recv,
            device_id=(g, peer), device_id_type=MESH,
        ).start()
        return c

    lax.fori_loop(1, n, send_sums, 0)

    with scope("left"):
        pass
    for direction, count in ((0, half), (1, half - 1)):
        drain(wall.at[0, :, pl.ds(0, count)], ring_send.at[direction])
    for part in range(4):
        drain(wall.at[part, :, pl.ds(0, chips)], sib_send.at[part])
    drain(wall.at[0, :, pl.ds(0, chips - 1)], x_send)
    drain(wall.at[0, :, pl.ds(0, chips - 1)], y_send)
    drain(wall.at[0, :, pl.ds(0, half - 1)], xr_send)
    drain(wall.at[0, :, pl.ds(0, half)], yr_send)
    drain(bias_all.at[pl.ds(0, n - 1)], bias_send)
    for i in range(ITEMS):
        drain(pack.at[i, pl.ds(0, n - 1)], qkv_send.at[i])
        drain(outb.at[i, pl.ds(0, n - 1)], ret_send.at[i])
    with scope("sums"):
        drain(sums_all.at[pl.ds(0, n - 1)], sums_recv)
    drain(sums_all.at[pl.ds(0, n - 1)], sums_send)

    totals = jnp.sum(sums_all[...], axis=0)
    count = float(img_local * n * PATCH)
    step_float = jnp.full((img_local, PATCH), step_index[0], jnp.int32).astype(f32)
    delta = sigma_at(1.0 - (step_float + 1.0) / NSTEPS) - sigma_at(1.0 - step_float / NSTEPS)
    for p in range(prompts):
        t = [totals[:, s * prompts + p : s * prompts + p + 1] for s in range(4)]
        std_cond = jnp.sqrt((t[1] - t[0] * t[0] / count) / (count - 1.0) + 1e-06)
        std_guided = jnp.sqrt((t[3] - t[2] * t[2] / count) / (count - 1.0) + 1e-06)
        ratio = std_cond / std_guided
        guided = guided_v[p]
        velocity = rescale_mix * ratio * guided + (1.0 - rescale_mix) * guided
        results[0, p] = velocity
        results[1, p] = latent[p] + delta * velocity


def body(
    y_size,
    groups,
    n,
    img_query,
    img_key,
    img_value,
    txt_key,
    txt_value,
    txt_len,
    slot_of,
    step_index,
    residual,
    modulation,
    out_weight,
    out_bias,
    expand_weight,
    expand_bias,
    contract_weight,
    contract_bias,
    final_weight,
    final_bias,
    latent,
):
    batch, img_local, d_model = img_query.shape
    prompts = batch // 2
    hidden_own = expand_weight.shape[0]
    per_seq = n // batch
    rows = batch * img_local
    hbm = pl.BlockSpec(memory_space=pl.ANY)
    dma = pltpu.SemaphoreType.DMA
    half = n // 4
    arrays = (
        img_query, img_key, img_value, txt_key, txt_value, expand_bias, txt_len,
        slot_of, step_index, residual, modulation.transpose(1, 0, 2), out_weight, out_bias, contract_bias,
        final_weight.T, final_bias, latent,
    )
    held = tuple((pltpu.SMEM if a.dtype == jnp.int32 else pltpu.VMEM)(a.shape, a.dtype) for a in arrays)
    results = pl.pallas_call(
        functools.partial(kernel, (groups, n, y_size, per_seq)),
        out_shape=jax.ShapeDtypeStruct((2, *latent.shape), f32),
        in_specs=[hbm, hbm, tuple(hbm for _ in arrays)],
        out_specs=pl.BlockSpec(memory_space=pltpu.VMEM),
        scratch_shapes=[
            held,
            pltpu.VMEM((4, 2, n, hidden_own, d_model // 4), bf16),
            pltpu.VMEM((ITEMS, n, 16, LANES), bf16),
            pltpu.VMEM((ITEMS, n, 16, LANES), bf16),
            pltpu.VMEM((ITEMS, n, 4, LANES), bf16),
            pltpu.VMEM((ITEMS, n, 4, LANES), bf16),
            pltpu.VMEM((rows, d_model), bf16),
            pltpu.VMEM((n, 1, LANES), f32),
            pltpu.VMEM((n, LANES), f32),
            pltpu.VMEM((n // CHUNK, 1, CHUNK * hidden_own), f32),
            pltpu.VMEM((n, 1, LANES), f32),
            pltpu.VMEM((batch, img_local, d_model), f32),
            pltpu.VMEM((rows, d_model), bf16),
            pltpu.VMEM((rows, d_model), f32),
            pltpu.VMEM((batch, img_local, PATCH), f32),
            pltpu.VMEM((prompts, img_local, PATCH), f32),
            dma((len(arrays),)),
            dma((4, 2)),
            dma((ITEMS,)),
            dma((ITEMS,)),
            dma((ITEMS,)),
            dma((ITEMS,)),
            dma((2, half + 1)),
            dma((2, half + 1)),
            dma((2, half + 1)),
            dma((2, half + 1)),
            dma((4,)),
            dma((2,)),
            dma((4,)),
            dma,
            dma,
            dma,
            dma,
            dma,
            dma,
            dma,
            dma,
        ],
        compiler_params=pltpu.CompilerParams(
            collective_id=0, has_side_effects=True, vmem_limit_bytes=60 * 1024 * 1024
        ),
    )(expand_weight, contract_weight, arrays)
    return results[0], results[1]


def solution(mesh):
    in_specs = (
        P("groups", "seq", None),
        P("groups", "seq", None),
        P("groups", "seq", None),
        P("groups", "seq", None),
        P("groups", "seq", None),
        P("groups"),
        P("groups"),
        P("groups"),
        P("groups", "seq", None),
        P("groups", None, None),
        P(),
        P(),
        P("seq", None),
        P("seq"),
        P("seq", None),
        P(),
        P(),
        P(),
        P("groups", "seq", None),
    )
    out_specs = (P("groups", "seq", None), P("groups", "seq", None))
    groups, n = mesh.shape["groups"], mesh.shape["seq"]
    bits = groups.bit_length() - 1
    y_size = 1 << (bits - bits // 2)
    return jax.shard_map(
        functools.partial(body, y_size, groups, n),
        mesh=mesh, in_specs=in_specs, out_specs=out_specs, check_vma=False,
    )
```

```python
import functools
import math

import jax
import jax.numpy as jnp
from jax import lax
from jax.experimental import pallas as pl
from jax.experimental.pallas import tpu as pltpu
from jax.sharding import PartitionSpec as P

HEADS = 24
HEAD_DIM = 64
PATCH = 64
NSTEPS = 28
ITEMS = 3
LANES = 128
MESH = pl.DeviceIdType.MESH

guidance_scale = 7.0
rescale_mix = 0.7
time_shift = 3.0

SENDS_PER_STEP = 13
ATTEND_AT = (7, 12, 17)
LAG = 3
CHUNK = 16

f32 = jnp.float32
bf16 = jnp.bfloat16


def sigma_at(time_value):
    return time_shift * time_value / (1.0 + (time_shift - 1.0) * time_value)


def roll(x, shift, axis):
    return pltpu.roll(x, shift, axis)


def modulate(values, shift, scale):
    centred = values - jnp.mean(values, axis=2, keepdims=True)
    variance = jnp.mean(centred * centred, axis=2, keepdims=True)
    return (centred * lax.rsqrt(variance + 1e-06) * (1.0 + scale) + shift)


def kernel(
    sizes,
    expand_weight, contract_weight, arrays, results, held,
    wall, pack, got, outb, back, attended, bias_all, bias_rows, bias_units, sums_all, hidden, ff_in, acc, pred_v, guided_v,
    in_sem, w_sem, qkv_send, qkv_recv, ret_send, ret_recv, own_recv, x_recv, y_recv, d_recv, sib_recv,
    ring_send, sib_send, x_send, y_send, xr_send, yr_send, bias_send, bias_recv, bias_sib_send, bias_sib_recv, sums_send, sums_recv,
):
    groups, n, y_size, per_seq = sizes
    (
        img_query, img_key, img_value, txt_key, txt_value, expand_bias, txt_len,
        slot_of, step_index, residual, modulation, ow_v, out_bias, contract_bias, final_weight, final_bias, latent,
    ) = held
    early = 7
    chips = n // 2
    half = chips // 2
    g = lax.axis_index("groups")
    me = lax.axis_index("seq")
    core = lax.rem(me, 2)
    sibling = me + 1 - 2 * core
    right = lax.rem(me + 2, n)
    left = lax.rem(me + n - 2, n)
    gy = lax.rem(g, 2)
    gx = lax.rem(g // y_size, 2)
    y_partner = g + 1 - 2 * gy
    x_partner = g + y_size * (1 - 2 * gx)
    q = 2 * gx + gy
    qx = 2 * (1 - gx) + gy
    qy = 2 * gx + 1 - gy
    qd = 3 - q
    width = wall.shape[-1]

    barrier = pltpu.get_barrier_semaphore()

    def peer_at(j):
        away = n // 2 + (1 - 2 * (j % 2)) * (j // 2)
        return me + away - n * (me + away >= n).astype(jnp.int32)

    def greet(j, c):
        pl.semaphore_signal(barrier, inc=1, device_id=(g, peer_at(j)), device_id_type=MESH)
        return c

    lax.fori_loop(1, n, greet, 0)
    pl.semaphore_signal(barrier, inc=1, device_id=(x_partner, me), device_id_type=MESH)
    pl.semaphore_signal(barrier, inc=1, device_id=(y_partner, me), device_id_type=MESH)

    in_copies = [pltpu.make_async_copy(a, h, in_sem.at[i]) for i, (a, h) in enumerate(zip(arrays, held))]
    for copy in in_copies:
        copy.start()
    own_copies = []
    for part in range(4):
        columns = pl.ds(part * width, width)
        own_copies.append(
            pltpu.make_async_copy(expand_weight.at[:, columns], wall.at[part, 0, me], w_sem.at[part, 0])
        )
        own_copies.append(
            pltpu.make_async_copy(contract_weight.at[:, columns], wall.at[part, 1, me], w_sem.at[part, 1])
        )
    for copy in own_copies:
        copy.start()
    for copy in in_copies[:early]:
        copy.wait()

    img_local = img_query.shape[1]
    batch = img_query.shape[0]
    lane = lax.broadcasted_iota(jnp.int32, (batch, 8, LANES), 2)
    sub = lax.broadcasted_iota(jnp.int32, (batch, 8, LANES), 1)
    low = sub < 4
    same = low == (lane < 64)

    def paired(x):
        return jnp.where(same, x, roll(roll(x, 64, 2), 4, 1))

    sub4 = lax.rem(sub, 4)
    for pair in range(HEADS // 2):
        cols = slice(pair * LANES, (pair + 1) * LANES)
        zq = paired(img_query[:, :, cols].astype(f32))
        zk = paired(img_key[:, :, cols].astype(f32))
        zv = paired(img_value[:, :, cols].astype(f32))
        tk = txt_key[:, :, cols].astype(f32)
        tv = txt_value[:, :, cols].astype(f32)
        t = jnp.concatenate([tk, tv], axis=1)
        swapped = roll(t, 64, 2)
        t_same = (sub4 < 2) == (lane < 64)
        zt = jnp.where(t_same, t, jnp.where(sub4 < 2, roll(swapped, 6, 1), roll(swapped, 2, 1)))
        t_even = jnp.where(sub < 6, roll(zt, 4, 1), roll(zt, 2, 1))
        t_odd = jnp.where(sub < 6, roll(zt, 2, 1), zt)
        for odd in range(2):
            head = 2 * pair + odd
            if odd == 0:
                top = jnp.where(low, zq, roll(zk, 4, 1))
                bottom = jnp.where(low, zv, t_even)
            else:
                top = jnp.where(low, roll(zq, 4, 1), zk)
                bottom = jnp.where(low, roll(zv, 4, 1), t_odd)
            block = jnp.concatenate([top, bottom], axis=1).astype(bf16)
            for b in range(batch):
                pack[head % ITEMS, per_seq * b + head // ITEMS] = block[b]

    my_b = me // per_seq
    my_k = lax.rem(me, per_seq)
    bias_all[me] = jnp.zeros((1, LANES), f32)
    bias_all[me, 0:1, 0 : expand_bias.shape[0]] = expand_bias[...].astype(f32).reshape(1, -1)
    for i in range(ITEMS):
        got[i, me] = pack[i, me]

    for copy in own_copies:
        copy.wait()
    with jax.named_scope("barrier"):
        pl.semaphore_wait(barrier, n + 1)

    def drain(ref, sem):
        pltpu.make_async_copy(ref, ref, sem).wait()

    scope = jax.named_scope

    def ring(slot, direction, k, to):
        return pltpu.make_async_remote_copy(
            wall.at[q, :, slot], wall.at[q, :, slot], ring_send.at[direction], own_recv.at[direction, k],
            device_id=(g, to), device_id_type=MESH,
        )

    def to_sibling(part, slot):
        return pltpu.make_async_remote_copy(
            wall.at[part, :, slot], wall.at[part, :, slot], sib_send.at[part], sib_recv.at[part],
            device_id=(g, sibling), device_id_type=MESH,
        )

    def across(part, slot, send, recv, partner):
        return pltpu.make_async_remote_copy(
            wall.at[part, :, slot], wall.at[part, :, slot], send, recv,
            device_id=(partner, me), device_id_type=MESH,
        )

    def slot_at(direction, k):
        if direction == 0:
            return lax.rem(me + n - 2 * k, n)
        return lax.rem(me + 2 * k, n)

    def bias_ring(slot, direction, k, to):
        return pltpu.make_async_remote_copy(
            bias_all.at[slot], bias_all.at[slot], bias_send.at[direction], bias_recv.at[direction, k],
            device_id=(g, to), device_id_type=MESH,
        )

    def bias_sibling(slot):
        return pltpu.make_async_remote_copy(
            bias_all.at[slot], bias_all.at[slot], bias_sib_send, bias_sib_recv,
            device_id=(g, sibling), device_id_type=MESH,
        )

    bias_ring(me, 0, 1, right).start()
    bias_ring(me, 1, 1, left).start()
    bias_sibling(me).start()
    ring(me, 0, 1, right).start()
    ring(me, 1, 1, left).start()
    for part in range(4):
        to_sibling(part, me).start()

    def send_item(index, c):
        i = sum((index >= at * (n - 1)).astype(jnp.int32) for at in range(1, ITEMS))
        peer = peer_at(index - i * (n - 1) + 1)
        pltpu.make_async_remote_copy(
            pack.at[i, peer], got.at[i, me], qkv_send.at[i], qkv_recv.at[i],
            device_id=(g, peer), device_id_type=MESH,
        ).start()
        return c

    def attend(i):
        with scope("items"):
            drain(got.at[i, pl.ds(0, n - 1)], qkv_recv.at[i])
        x = got[i].astype(f32)
        top = x[:, 0:8, :].reshape(n // 2, 2, 8, LANES)
        bottom = x[:, 8:16, :].reshape(n // 2, 2, 8, LANES)
        sub_ = lax.broadcasted_iota(jnp.int32, (n // 2, 8, LANES), 1)
        a, b = top[:, 0], top[:, 1]
        c, d = bottom[:, 0], bottom[:, 1]
        qs = jnp.where(sub_ < 4, a, roll(b, 4, 1)).reshape(4 * n, LANES)
        ks = jnp.where(sub_ < 4, roll(a, 4, 1), b).reshape(4 * n, LANES)
        vs = jnp.where(sub_ < 4, c, roll(d, 4, 1)).reshape(4 * n, LANES)
        t = jnp.where(sub_ < 4, roll(c, 4, 1), d).reshape(n // 4, 2, 8, LANES)
        t0, t1 = t[:, 0], t[:, 1]
        sub_t = lax.rem(lax.broadcasted_iota(jnp.int32, (n // 4, 8, LANES), 1), 4)
        tks = jnp.where(sub_t < 2, t0, roll(t1, 2, 1)).reshape(2 * n, LANES)
        tvs = jnp.where(sub_t < 2, roll(t0, 6, 1), t1).reshape(2 * n, LANES)
        kk = jnp.concatenate([ks, tks], axis=0)
        vv = jnp.concatenate([vs, tvs], axis=0)
        keys = jnp.concatenate([kk, roll(kk, 64, 1)], axis=0).astype(bf16)
        vals = jnp.concatenate([vv, roll(vv, 64, 1)], axis=0).astype(bf16)
        img, rows = 4 * n, 6 * n
        m = lax.broadcasted_iota(jnp.int32, (1, 2 * n), 1)
        s8 = m % 8
        token = 4 * (4 * (m // 8) + 2 * ((s8 % 4) // 2) + s8 // 4) + m % 2
        length = txt_len[my_b]
        lane_q = lax.broadcasted_iota(jnp.int32, (4 * n, LANES), 1)
        scale = 1.0 / math.sqrt(HEAD_DIM)
        outs = []
        for side in range(2):
            inside = (lane_q < 64) if side == 0 else (lane_q >= 64)
            qa = jnp.where(inside, qs * scale, 0.0).astype(bf16)
            scores = lax.dot_general(qa, keys, (((1,), (1,)), ((), ())), preferred_element_type=f32)
            pieces = []
            for swap in range(2):
                which = swap if side == 0 else 1 - swap
                pieces.append(scores[:, swap * rows : swap * rows + img])
                text = scores[:, swap * rows + img : (swap + 1) * rows]
                pieces.append(jnp.where(token + 2 * which < length, text, -jnp.inf))
            scores = jnp.concatenate(pieces, axis=1)
            top_score = jnp.max(scores, axis=1, keepdims=True)
            expon = jnp.exp(scores - top_score)
            weights = (expon * (1.0 / jnp.sum(expon, axis=1, keepdims=True))).astype(bf16)
            outs.append(jnp.dot(weights, vals, preferred_element_type=f32))
        both = jnp.where(lane_q < 64, outs[0], outs[1]).reshape(n // 2, 8, LANES).astype(bf16)
        outb[i] = jnp.stack([both[:, 0:4], both[:, 4:8]], axis=1).reshape(n, 4, LANES)

        def send_back(j, carry):
            peer = peer_at(j)
            pltpu.make_async_remote_copy(
                outb.at[i, peer], back.at[i, me], ret_send.at[i], ret_recv.at[i],
                device_id=(g, peer), device_id_type=MESH,
            ).start()
            return carry

        lax.fori_loop(1, n, send_back, 0)
        back[i, me] = outb[i, me]

    def step(k, carry):
        total = ITEMS * (n - 1)
        first = (k - 1) * SENDS_PER_STEP

        @pl.when(first < total)
        def _():
            with scope("send"):
                lax.fori_loop(first, jnp.minimum(first + SENDS_PER_STEP, total), send_item, 0)

        for direction, last, onward in ((0, half, right), (1, half - 1, left)):

            @pl.when(k <= last)
            def _():
                slot = slot_at(direction, k)
                with scope("own"):
                    ring(slot, direction, k, onward).wait_recv()
                    bias_ring(slot, direction, k, onward).wait_recv()

                @pl.when(k < last)
                def _():
                    ring(slot, direction, k + 1, onward).start()
                    bias_ring(slot, direction, k + 1, onward).start()

                across(q, slot, x_send, x_recv.at[direction, k], x_partner).start()
                across(q, slot, y_send, y_recv.at[direction, k], y_partner).start()
                to_sibling(q, slot).start()
                bias_sibling(slot).start()

        for direction, last in ((0, half), (1, half - 1)):
            late = k - LAG

            @pl.when((late >= 1) & (late <= last))
            def _():
                slot = slot_at(direction, late)
                with scope("x"):
                    across(qx, slot, x_send, x_recv.at[direction, late], x_partner).wait_recv()
                if direction == 0:
                    across(qx, slot, yr_send, d_recv.at[direction, late], y_partner).start()
                to_sibling(qx, slot).start()
                with scope("y"):
                    across(qy, slot, y_send, y_recv.at[direction, late], y_partner).wait_recv()
                if direction == 1:
                    across(qy, slot, xr_send, d_recv.at[direction, late], x_partner).start()
                to_sibling(qy, slot).start()

            later = k - 2 * LAG

            @pl.when((later >= 1) & (later <= last))
            def _():
                slot = slot_at(direction, later)
                with scope("d"):
                    across(qd, slot, xr_send, d_recv.at[direction, later], x_partner).wait_recv()
                to_sibling(qd, slot).start()

        first_at, second_at, third_at = ATTEND_AT

        @pl.when((k == first_at) | (k == second_at) | (k == third_at))
        def _():
            with scope("attend"):
                attend((k >= second_at).astype(jnp.int32) + (k >= third_at).astype(jnp.int32))

        return carry

    lax.fori_loop(1, half + 2 * LAG + 1, step, 0)

    chunks = len(range(0, n, CHUNK))
    hidden_own = wall.shape[3]
    chunk_units = CHUNK * hidden_own
    drain(bias_all.at[pl.ds(0, chips)], bias_sib_recv)
    for r in range(n):
        bias_rows[r : r + 1, :] = bias_all[r]
    unit = lax.broadcasted_iota(jnp.int32, (LANES, chunk_units), 1)
    block_of = ((unit.astype(f32) + 0.5) * (1.0 / hidden_own)).astype(jnp.int32)
    pick = jnp.where(
        unit - block_of * hidden_own == lax.broadcasted_iota(jnp.int32, (LANES, chunk_units), 0), 1.0, 0.0
    ).astype(bf16)
    mine = block_of[:CHUNK] == lax.broadcasted_iota(jnp.int32, (CHUNK, chunk_units), 0)
    for c in range(chunks):
        spread = jnp.dot(
            bias_rows[c * CHUNK : (c + 1) * CHUNK, :].astype(bf16), pick, preferred_element_type=f32
        )
        bias_units[c] = jnp.sum(jnp.where(mine, spread, 0.0), axis=0, keepdims=True)

    for i in range(ITEMS):
        with scope("ret"):
            drain(back.at[i, pl.ds(0, n - 1)], ret_recv.at[i])
    for pair in range(HEADS // 2):
        cols = slice(pair * LANES, (pair + 1) * LANES)
        halves = []
        for head in (2 * pair, 2 * pair + 1):
            i, k = head % ITEMS, head // ITEMS
            halves.append(jnp.stack([back[i, per_seq * b + k].astype(f32) for b in range(batch)], axis=0))
        z = jnp.concatenate(halves, axis=1)
        attended[:, cols] = paired(z).reshape(batch * img_local, LANES).astype(bf16)

    for copy in in_copies[early:]:
        copy.wait()
    d_model = attended.shape[-1]
    shape3 = (batch, img_local, d_model)
    projected = jnp.dot(attended[...], ow_v[...], preferred_element_type=f32).reshape(shape3) + out_bias[...].reshape(1, 1, -1)
    hidden[...] = residual[...].astype(f32) + modulation[0][:, None, :] * projected
    ff_in[...] = (
        modulate(hidden[...], modulation[1][:, None, :], modulation[2][:, None, :])
        .reshape(batch * img_local, d_model)
        .astype(bf16)
    )
    for part in range(4):
        with scope("sib"):
            drain(wall.at[part, :, pl.ds(0, chips)], sib_recv.at[part])

    for c in range(chunks):
        blocks = pl.ds(c * CHUNK, CHUNK)
        pre = bias_units[c]
        for side in range(2):
            w = jnp.concatenate(
                [wall[part, 0, blocks].reshape(chunk_units, width) for part in (2 * side, 2 * side + 1)], axis=1
            )
            pre = pre + lax.dot_general(
                ff_in[:, 2 * side * width : 2 * (side + 1) * width], w,
                (((1,), (1,)), ((), ())), preferred_element_type=f32,
            )
        act = (0.5 * pre * (1.0 + jnp.tanh(math.sqrt(2.0 / math.pi) * (pre + 0.044715 * pre * pre * pre)))).astype(bf16)
        for side in range(2):
            w = jnp.concatenate(
                [wall[part, 1, blocks].reshape(chunk_units, width) for part in (2 * side, 2 * side + 1)], axis=1
            )
            columns = slice(2 * side * width, 2 * (side + 1) * width)
            product = jnp.dot(act, w, preferred_element_type=f32)
            acc[:, columns] = product if c == 0 else acc[:, columns] + product


    ff_hidden = hidden[...] + modulation[3][:, None, :] * (acc[...].reshape(shape3) + contract_bias[...].reshape(1, 1, -1))
    normed = (
        modulate(ff_hidden, modulation[4][:, None, :], modulation[5][:, None, :])
        .reshape(batch * img_local, d_model)
        .astype(bf16)
    )
    pred = lax.dot_general(
        normed, final_weight[...], (((1,), (1,)), ((), ())), preferred_element_type=f32
    ) + final_bias[...].reshape(1, -1)
    pred_v[...] = pred.reshape(batch, img_local, PATCH)
    prompts = batch // 2
    lane_row = lax.broadcasted_iota(jnp.int32, (1, LANES), 1)
    row = jnp.zeros((1, LANES), f32)

    def full_sum(x):
        return jnp.sum(jnp.sum(x, axis=1, keepdims=True), axis=0, keepdims=True)

    for p in range(prompts):
        cond = pred_v[slot_of[p]]
        uncond = pred_v[slot_of[prompts + p]]
        guided = uncond + guidance_scale * (cond - uncond)
        guided_v[p] = guided
        for s, value in enumerate((cond, cond * cond, guided, guided * guided)):
            row = jnp.where(lane_row == s * prompts + p, full_sum(value), row)
    sums_all[me] = row

    def send_sums(j, c):
        peer = peer_at(j)
        pltpu.make_async_remote_copy(
            sums_all.at[me], sums_all.at[me], sums_send, sums_recv,
            device_id=(g, peer), device_id_type=MESH,
        ).start()
        return c

    lax.fori_loop(1, n, send_sums, 0)

    values = float(img_local * n * PATCH)
    step_float = jnp.full((img_local, PATCH), step_index[0], jnp.int32).astype(f32)
    delta = sigma_at(1.0 - (step_float + 1.0) / NSTEPS) - sigma_at(1.0 - step_float / NSTEPS)
    for direction, count in ((0, half), (1, half - 1)):
        drain(wall.at[0, :, pl.ds(0, count)], ring_send.at[direction])
    for part in range(4):
        drain(wall.at[part, :, pl.ds(0, chips)], sib_send.at[part])
    drain(wall.at[0, :, pl.ds(0, chips - 1)], x_send)
    drain(wall.at[0, :, pl.ds(0, chips - 1)], y_send)
    drain(wall.at[0, :, pl.ds(0, half - 1)], xr_send)
    drain(wall.at[0, :, pl.ds(0, half)], yr_send)
    for direction, count in ((0, half), (1, half - 1)):
        drain(bias_all.at[pl.ds(0, count)], bias_send.at[direction])
    drain(bias_all.at[pl.ds(0, chips)], bias_sib_send)
    for i in range(ITEMS):
        drain(pack.at[i, pl.ds(0, n - 1)], qkv_send.at[i])
        drain(outb.at[i, pl.ds(0, n - 1)], ret_send.at[i])
    with scope("sums"):
        drain(sums_all.at[pl.ds(0, n - 1)], sums_recv)
    drain(sums_all.at[pl.ds(0, n - 1)], sums_send)

    totals = jnp.sum(sums_all[...], axis=0)
    for p in range(prompts):
        t = [totals[:, s * prompts + p : s * prompts + p + 1] for s in range(4)]
        std_cond = jnp.sqrt((t[1] - t[0] * t[0] / values) / (values - 1.0) + 1e-06)
        std_guided = jnp.sqrt((t[3] - t[2] * t[2] / values) / (values - 1.0) + 1e-06)
        ratio = std_cond / std_guided
        guided = guided_v[p]
        velocity = rescale_mix * ratio * guided + (1.0 - rescale_mix) * guided
        results[0, p] = velocity
        results[1, p] = latent[p] + delta * velocity


def body(
    y_size,
    groups,
    n,
    img_query,
    img_key,
    img_value,
    txt_key,
    txt_value,
    txt_len,
    slot_of,
    step_index,
    residual,
    modulation,
    out_weight,
    out_bias,
    expand_weight,
    expand_bias,
    contract_weight,
    contract_bias,
    final_weight,
    final_bias,
    latent,
):
    batch, img_local, d_model = img_query.shape
    prompts = batch // 2
    hidden_own = expand_weight.shape[0]
    per_seq = n // batch
    rows = batch * img_local
    hbm = pl.BlockSpec(memory_space=pl.ANY)
    dma = pltpu.SemaphoreType.DMA
    half = n // 4
    arrays = (
        img_query, img_key, img_value, txt_key, txt_value, expand_bias, txt_len,
        slot_of, step_index, residual, modulation.transpose(1, 0, 2), out_weight, out_bias, contract_bias,
        final_weight.T, final_bias, latent,
    )
    held = tuple((pltpu.SMEM if a.dtype == jnp.int32 else pltpu.VMEM)(a.shape, a.dtype) for a in arrays)
    results = pl.pallas_call(
        functools.partial(kernel, (groups, n, y_size, per_seq)),
        out_shape=jax.ShapeDtypeStruct((2, *latent.shape), f32),
        in_specs=[hbm, hbm, tuple(hbm for _ in arrays)],
        out_specs=pl.BlockSpec(memory_space=pltpu.VMEM),
        scratch_shapes=[
            held,
            pltpu.VMEM((4, 2, n, hidden_own, d_model // 4), bf16),
            pltpu.VMEM((ITEMS, n, 16, LANES), bf16),
            pltpu.VMEM((ITEMS, n, 16, LANES), bf16),
            pltpu.VMEM((ITEMS, n, 4, LANES), bf16),
            pltpu.VMEM((ITEMS, n, 4, LANES), bf16),
            pltpu.VMEM((rows, d_model), bf16),
            pltpu.VMEM((n, 1, LANES), f32),
            pltpu.VMEM((n, LANES), f32),
            pltpu.VMEM((n // CHUNK, 1, CHUNK * hidden_own), f32),
            pltpu.VMEM((n, 1, LANES), f32),
            pltpu.VMEM((batch, img_local, d_model), f32),
            pltpu.VMEM((rows, d_model), bf16),
            pltpu.VMEM((rows, d_model), f32),
            pltpu.VMEM((batch, img_local, PATCH), f32),
            pltpu.VMEM((prompts, img_local, PATCH), f32),
            dma((len(arrays),)),
            dma((4, 2)),
            dma((ITEMS,)),
            dma((ITEMS,)),
            dma((ITEMS,)),
            dma((ITEMS,)),
            dma((2, half + 1)),
            dma((2, half + 1)),
            dma((2, half + 1)),
            dma((2, half + 1)),
            dma((4,)),
            dma((2,)),
            dma((4,)),
            dma,
            dma,
            dma,
            dma,
            dma((2,)),
            dma((2, half + 1)),
            dma,
            dma,
            dma,
            dma,
        ],
        compiler_params=pltpu.CompilerParams(
            collective_id=0, has_side_effects=True, vmem_limit_bytes=60 * 1024 * 1024
        ),
    )(expand_weight, contract_weight, arrays)
    return results[0], results[1]


def solution(mesh):
    in_specs = (
        P("groups", "seq", None),
        P("groups", "seq", None),
        P("groups", "seq", None),
        P("groups", "seq", None),
        P("groups", "seq", None),
        P("groups"),
        P("groups"),
        P("groups"),
        P("groups", "seq", None),
        P("groups", None, None),
        P(),
        P(),
        P("seq", None),
        P("seq"),
        P("seq", None),
        P(),
        P(),
        P(),
        P("groups", "seq", None),
    )
    out_specs = (P("groups", "seq", None), P("groups", "seq", None))
    groups, n = mesh.shape["groups"], mesh.shape["seq"]
    bits = groups.bit_length() - 1
    y_size = 1 << (bits - bits // 2)
    return jax.shard_map(
        functools.partial(body, y_size, groups, n),
        mesh=mesh, in_specs=in_specs, out_specs=out_specs, check_vma=False,
    )
```
